32 devices in a mesh: cuts: 4 (over z), dev: 8 (over y, x, core).
Axes of the slice: x: 2, y: 2, z: 4, core: 2. Of those that a mesh axis runs over, the one named last changes fastest.
Arguments:
- inputs: bfloat16 [16384, 3072], P(('cuts', 'dev')), may hold values from -6 to 6
- cotangent: bfloat16 [16384, 512], P(('cuts', 'dev')), may hold values from -0.29882812 to 0.29882812
- errors: bfloat16 [32, 3072, 512], P(('cuts', 'dev')), may hold values from -6 to 6
- previous_q: float32 [512, 64], replicated, may hold values from -0.25 to 0.25
Outputs:
- new_errors: bfloat16 [32, 3072, 512], P(('cuts', 'dev'))
- p_hat: float32 [3072, 64], replicated
- q_mean: float32 [512, 64], replicated
The draws below stay inside these ranges and needn't reach their ends.
All inputs are finite; a program needn't handle non-finite values.
Results may differ from the reference program's by a relative error of at most 0.001.
Values sent between devices are 32-bit elements; how exact they have to be, the bound alone decides.
No kernel may reach another device: no remote copies, remote signals or barrier semaphores. Data moves between devices by JAX's collectives and lax.ppermute only.
A program may use at most 64 MiB of HBM per device.

```python
import jax
import jax.numpy as jnp
from jax import lax

D = 3072
KVW = 512
RANK = 64
TOK_DEV = 512
TOKENS = 16384
N_CUTS = 4
N_DEV = 8
DEVICES = 32


def block_scale(key, extent, cuts, low, high):
    def one(axis_at, shards_of):
        steps = jax.random.uniform(jax.random.fold_in(jax.random.fold_in(key, 6), axis_at), (shards_of,), jnp.float32, low / len(cuts), high / len(cuts))
        return jnp.repeat(jnp.exp(steps), extent[axis_at] // shards_of).reshape((-1,) + (1,) * (len(extent) - axis_at - 1))

    loudness = one(*cuts[0])
    for cut in cuts[1:]:
        loudness = loudness * one(*cut)
    return loudness


def gaussian(rng, dims, width, bound, cuts=(), held_as=jnp.bfloat16):
    drawn = jax.random.normal(rng, dims, jnp.float32) * width
    if len(cuts) > 0:
        drawn = block_scale(rng, dims, cuts, -0.22, 0.18) * drawn
    return jnp.clip(drawn, min=-bound, max=bound).astype(held_as)


def setup_inputs(seed: int = 0) -> dict:
    key_of = jax.random.split(jax.random.key(seed), 5)
    return {
        "inputs": gaussian(key_of[0], (TOKENS, D), 1.0, 6.0, ((0, 32),)),
        "cotangent": gaussian(key_of[1], (TOKENS, KVW), 0.05, 0.29882812, ((0, 32),)),
        "errors": gaussian(key_of[2], (DEVICES, D, KVW), 1.0, 6.0, ((0, 32),)),
        "previous_q": gaussian(key_of[3], (KVW, RANK), KVW ** -0.5, 0.25, (), jnp.float32),
    }


HI = lax.Precision.HIGHEST

def orthonormal(p_sum):
    gram = jnp.dot(p_sum.T, p_sum, precision=HI)
    lower = jnp.linalg.cholesky(gram)
    return lax.linalg.triangular_solve(lower, p_sum, left_side=False, lower=True, transpose_a=True)

def reference(inputs, cotangent, errors, previous_q):
    count = N_CUTS * N_DEV
    xs = inputs.reshape(count, TOK_DEV, D)
    ys = cotangent.reshape(count, TOK_DEV, KVW)

    def p_step(acc, triple):
        xw, yw, ew = triple
        xf = xw.astype(jnp.float32)
        yf = yw.astype(jnp.float32)
        term = jnp.dot(xf.T, jnp.dot(yf, previous_q, precision=HI), precision=HI)
        term = term + jnp.dot(ew.astype(jnp.float32), previous_q, precision=HI)
        return (acc + term, None)
    p_sum, _ = lax.scan(p_step, jnp.zeros((D, RANK), jnp.float32), (xs, ys, errors))
    p_hat = orthonormal(p_sum)

    def q_step(acc, triple):
        xw, yw, ew = triple
        xf = xw.astype(jnp.float32)
        yf = yw.astype(jnp.float32)
        term = jnp.dot(yf.T, jnp.dot(xf, p_hat, precision=HI), precision=HI)
        term = term + jnp.dot(ew.astype(jnp.float32).T, p_hat, precision=HI)
        return (acc + term, None)
    q_sum, _ = lax.scan(q_step, jnp.zeros((KVW, RANK), jnp.float32), (xs, ys, errors))
    q_mean = q_sum / count
    approx = jnp.dot(p_hat, q_mean.T, precision=HI)

    def refresh(triple):
        xw, yw, ew = triple
        merged = jnp.dot(xw.astype(jnp.float32).T, yw.astype(jnp.float32), precision=HI) + ew.astype(jnp.float32)
        return (merged - approx).astype(jnp.bfloat16)
    new_errors = lax.map(refresh, (xs, ys, errors))
    return (new_errors, p_hat, q_mean)
```

```python
import functools

import jax
import jax.numpy as jnp
from jax import lax
from jax.experimental import pallas as pl
from jax.experimental.pallas import tpu as pltpu
from jax.sharding import Mesh, PartitionSpec as P

HI = lax.Precision.HIGHEST
F32 = jnp.float32
BF16 = jnp.bfloat16
LANES = 128
VM = pl.BlockSpec(memory_space=pltpu.VMEM)
ANY = pl.BlockSpec(memory_space=pl.ANY)
SM = pl.BlockSpec(memory_space=pltpu.SMEM)
NN = (((1,), (0,)), ((), ()))
NT = (((1,), (1,)), ((), ()))
TN = (((0,), (0,)), ((), ()))


def dot(a, b, dims, precision=None):
    return lax.dot_general(a, b, dims, precision=precision, preferred_element_type=F32)


def split3(x):
    high = x.astype(BF16)
    rest = x - high.astype(F32)
    mid = rest.astype(BF16)
    low = (rest - mid.astype(F32)).astype(BF16)
    return jnp.concatenate([high, mid, low], axis=0)


def fold3(x):
    rows = x.shape[0] // 3
    return x[:rows] + x[rows : 2 * rows] + x[2 * rows :]


def call(kernel, outs, ins_specs, out_specs, scratch, args, name, flops, limit=24):
    return pl.pallas_call(
        kernel,
        out_shape=outs,
        in_specs=ins_specs,
        out_specs=out_specs,
        scratch_shapes=scratch,
        compiler_params=pltpu.CompilerParams(vmem_limit_bytes=limit * 1024 * 1024),
        cost_estimate=pl.CostEstimate(flops=flops, bytes_accessed=0, transcendentals=0),
        name=name,
    )(*args)


def vmem(shape, dtype=F32):
    return jax.ShapeDtypeStruct(shape, dtype)


def left_kernel(pieces, block, ids, x_hbm, y_hbm, e_hbm, q_ref, keep, send, xv, yv, ev, v3, total, sem):
    depth = x_hbm.shape[1]
    rank = q_ref.shape[1]
    steps = depth // block
    y_copy = pltpu.make_async_copy(y_hbm, yv, sem.at[0])
    y_copy.start()
    x_copies, e_copies = [], []
    for i in range(steps):
        cut = pl.ds(i * block, block)
        x_copies.append(pltpu.make_async_copy(x_hbm.at[:, cut], xv.at[:, cut], sem.at[1 + 2 * i]))
        e_copies.append(pltpu.make_async_copy(e_hbm.at[0, cut, :], ev.at[cut, :], sem.at[2 + 2 * i]))
        x_copies[i].start()
        e_copies[i].start()
    q3 = split3(q_ref[...].T)
    y_copy.wait()
    v3[...] = split3(fold3(dot(q3, yv[...], NT)))
    for i in range(steps):
        cut = pl.ds(i * block, block)
        x_copies[i].wait()
        e_copies[i].wait()
        part = fold3(dot(v3[...], xv[:, cut], NN) + dot(q3, ev[cut, :], NT))
        for j in range(block // LANES):
            at = (i * (block // LANES) + j) * rank
            total[at : at + rank, :] = part[:, j * LANES : (j + 1) * LANES]
    place(pieces, ids, total, (keep, send))


def place(pieces, ids, total, outs):
    cores, chips, cuts = pieces
    size = total.shape[0] // (cores * chips * cuts)
    for core in range(cores):
        for chip in range(chips):
            for cut in range(cuts):
                chunk = ((core ^ ids[0]) * chips + (chip ^ ids[1])) * cuts + (cut ^ ids[2])
                at = (chip * cuts + cut) * size
                start = pl.multiple_of(chunk * size, 8)
                outs[core][at : at + size, :] = total[pl.ds(start, size), :]


def sum_kernel(count, *refs):
    ins, outs = refs[:count], refs[count:]
    size = outs[0].shape[0]
    for k, out in enumerate(outs):
        rows = pl.ds(k * size, size)
        total = ins[0][rows, :]
        for other in ins[1:]:
            total = total + other[rows, :]
        out[...] = total


def add_up(ins, pieces, name):
    rows = ins[0].shape[0]
    shape = vmem((rows // pieces, LANES))
    return call(
        functools.partial(sum_kernel, len(ins)), [shape] * pieces, [VM] * len(ins), [VM] * pieces, [], ins, name, 10**7, 8
    )


def join_kernel(*refs):
    out = refs[-1]
    size = refs[0].shape[0]
    for k, part in enumerate(refs[:-1]):
        out[k * size : (k + 1) * size, :] = part[...]


def join(parts, name):
    if len(parts) == 1:
        return parts[0]
    shape = vmem((parts[0].shape[0] * len(parts), LANES))
    return call(join_kernel, shape, [VM] * len(parts), VM, [], parts, name, 10**7, 8)


def right_kernel(pieces, ids, *refs):
    cores, chips, cuts = pieces
    parts = refs[: cores * chips]
    xv, yv, ev, keep, send, left, p3, total = refs[cores * chips :]
    rank = p3.shape[0] // 3
    size = left.shape[0] // (cores * chips * cuts)
    for core in range(cores):
        for chip in range(chips):
            for cut in range(cuts):
                chunk = ((core ^ ids[0]) * chips + (chip ^ ids[1])) * cuts + (cut ^ ids[2])
                start = pl.multiple_of(chunk * size, 8)
                left[pl.ds(start, size), :] = parts[core * chips + chip][cut * size : (cut + 1) * size, :]
    for c in range(left.shape[0] // rank):
        p3[:, c * LANES : (c + 1) * LANES] = split3(left[c * rank : (c + 1) * rank, :])
    u3 = split3(fold3(dot(p3[...], xv[...], NT)))
    right = fold3(dot(p3[...], ev[...], NN) + dot(u3, yv[...], NN))
    for c in range(right.shape[1] // LANES):
        total[c * rank : (c + 1) * rank, :] = right[:, c * LANES : (c + 1) * LANES]
    place((cores, 1, 1), (ids[0], 0, 0), total, (keep, send))


def merge_kernel(block, xv, yv, ev, merged):
    for i in range(ev.shape[0] // block):
        cut = pl.ds(i * block, block)
        merged[cut, :] = dot(xv[:, cut], yv[...], TN) + ev[cut, :].astype(F32)


def factor_kernel(left, lower_inv, wide):
    rank = lower_inv.shape[0]
    for c in range(left.shape[0] // rank):
        wide[:, c * LANES : (c + 1) * LANES] = left[c * rank : (c + 1) * rank, :]
    gram = dot(wide[...], wide[...], NT, HI)
    row = lax.broadcasted_iota(jnp.int32, (rank, 2 * rank), 0)
    lane = lax.broadcasted_iota(jnp.int32, (rank, 2 * rank), 1)
    eye = jnp.where(lane - rank == row, 1.0, 0.0).astype(F32)
    work = jnp.where(lane < rank, jnp.concatenate([gram, gram], axis=1), eye)
    groups = [work[8 * g : 8 * g + 8, :] for g in range(rank // 8)]
    sub = lax.broadcasted_iota(jnp.int32, (8, 2 * rank), 0)
    for k in range(rank):
        g, s = divmod(k, 8)
        pivot = groups[g][s : s + 1, :]
        scaled = pivot / pivot[:, k : k + 1]
        for h in range(g, rank // 8):
            update = groups[h][:, k : k + 1] * scaled
            if h == g:
                update = jnp.where(sub > s, update, 0.0)
            groups[h] = groups[h] - update
    for g in range(rank // 8):
        diag = jnp.sum(jnp.where(lane[8 * g : 8 * g + 8] == row[8 * g : 8 * g + 8], groups[g], 0.0), axis=1, keepdims=True)
        lower_inv[8 * g : 8 * g + 8, :] = groups[g][:, rank:] / jnp.sqrt(diag)


def hat_kernel(left, lower_inv, p_hat, hat3):
    rank = lower_inv.shape[0]
    inv = lower_inv[...]
    for c in range(left.shape[0] // rank):
        block = left[c * rank : (c + 1) * rank, :]
        hat = dot(block, inv, (((0,), (1,)), ((), ())), HI)
        rows = slice(c * LANES, (c + 1) * LANES)
        p_hat[rows, :] = hat
        high = hat.astype(BF16)
        low = (hat - high.astype(F32)).astype(BF16)
        hat3[rows, :] = jnp.concatenate([high, low, high], axis=1)


def last_kernel(devices, block, ids, keep, other, lower_inv, hat3, merged, new_errors, q_mean, total, out, sem):
    rank = lower_inv.shape[0]
    half = keep.shape[0]
    total[pl.ds(pl.multiple_of(ids[0] * half, 8), half), :] = keep[...]
    if other is not None:
        total[pl.ds(pl.multiple_of((1 - ids[0]) * half, 8), half), :] = other[...]
    wide = jnp.concatenate([total[c * rank : (c + 1) * rank, :] for c in range(total.shape[0] // rank)], axis=1)
    right = dot(lower_inv[...], wide, NN, HI) / devices
    high = right.astype(BF16)
    low = (right - high.astype(F32)).astype(BF16)
    q3 = jnp.concatenate([high, high, low], axis=0)
    copies = []
    for i in range(merged.shape[0] // block):
        cut = pl.ds(i * block, block)
        out[cut, :] = (merged[cut, :] - dot(hat3[cut, :], q3, NN)).astype(BF16)
        copies.append(pltpu.make_async_copy(out.at[cut, :], new_errors.at[0, cut, :], sem.at[i]))
        copies[i].start()
    q_mean[...] = right.T
    for copy in copies:
        copy.wait()


def swap(x, axis, size, by):
    return lax.ppermute(x, axis, [(i, i ^ by) for i in range(size)])


def body(sizes, inputs, cotangent, errors, previous_q):
    cores, chips, cuts = sizes
    tokens, depth = inputs.shape
    width, rank = previous_q.shape
    devices = cores * chips * cuts
    rows = depth * rank // LANES
    block = next(b for b in (512, 384, 256, LANES) if depth % b == 0)
    steps = depth // block
    share = rows // (cores * chips)
    scatter = cuts if share % (8 * cuts) == 0 else 1
    pieces = (cores, chips, scatter)
    ids = jnp.stack(
        [lax.axis_index("core"), lax.axis_index("chip"), lax.axis_index("cuts") if scatter > 1 else 0]
    ).astype(jnp.int32)
    half = vmem((rows // cores, LANES))
    keep, send, xv, yv, ev = call(
        functools.partial(left_kernel, pieces, block),
        [half, half, vmem((tokens, depth), BF16), vmem((tokens, width), BF16), vmem((depth, width), BF16)],
        [SM, ANY, ANY, ANY, VM],
        [VM] * 5,
        [
            pltpu.VMEM((3 * rank, tokens), BF16),
            pltpu.VMEM((rows, LANES), F32),
            pltpu.SemaphoreType.DMA((1 + 2 * steps,)),
        ],
        (ids, inputs, cotangent, errors, previous_q),
        "left",
        6 * devices * 10**7,
        20,
    )
    got = swap(send, "core", cores, 1)
    parts = add_up([keep, got], chips, "sum_core")
    got = [parts[0]] + [swap(parts[k], "chip", chips, k) for k in range(1, chips)]
    parts = add_up(got, scatter, "sum_chip")
    if scatter > 1:
        got = [parts[0]] + [swap(parts[k], "cuts", cuts, k) for k in range(1, cuts)]
        mine = add_up(got, 1, "sum_cut")[0]
        mine = join([mine] + [swap(mine, "cuts", cuts, k) for k in range(1, cuts)], "join_cut")
    else:
        mine = add_up([parts[0]] + [swap(parts[0], "cuts", cuts, k) for k in range(1, cuts)], 1, "sum_cut")[0]
    parts = [mine] + [swap(mine, "chip", chips, k) for k in range(1, chips)]
    parts = parts + [swap(part, "core", cores, 1) for part in parts]

    merged = call(
        functools.partial(merge_kernel, block),
        vmem((depth, width)),
        [VM] * 3,
        VM,
        [],
        (xv, yv, ev),
        "merge",
        2 * tokens * depth * width,
        8,
    )
    half = vmem((width * rank // LANES // cores, LANES))
    keep, send, left = call(
        functools.partial(right_kernel, pieces),
        [half, half, vmem((rows, LANES))],
        [SM] + [VM] * (len(parts) + 3),
        [VM] * 3,
        [pltpu.VMEM((3 * rank, depth), BF16), pltpu.VMEM((width * rank // LANES, LANES), F32)],
        (ids, *parts, xv, yv, ev),
        "right",
        10**9,
        16,
    )
    got = swap(send, "core", cores, 1)
    part = add_up([keep, got], 1, "sum_core")[0]
    part = add_up([part] + [swap(part, "chip", chips, k) for k in range(1, chips)], 1, "sum_chip")[0]
    part = add_up([part] + [swap(part, "cuts", cuts, k) for k in range(1, cuts)], 1, "sum_cut")[0]
    other = swap(part, "core", cores, 1)

    lower_inv = call(
        factor_kernel, vmem((rank, rank)), [VM], VM, [pltpu.VMEM((rank, depth), F32)], (left,), "factor", 10**9, 8
    )
    p_hat, hat3 = call(
        hat_kernel,
        [vmem((depth, rank)), vmem((depth, 3 * rank), BF16)],
        [VM, VM],
        [VM, VM],
        [],
        (left, lower_inv),
        "hat",
        10**9,
        8,
    )
    new_errors, q_mean = call(
        functools.partial(last_kernel, devices, block),
        [vmem((1, depth, width), BF16), vmem((width, rank))],
        [SM] + [VM] * 5,
        [ANY, VM],
        [
            pltpu.VMEM((width * rank // LANES, LANES), F32),
            pltpu.VMEM((depth, width), BF16),
            pltpu.SemaphoreType.DMA((steps,)),
        ],
        (ids, part, other, lower_inv, hat3, merged),
        "last",
        10**9,
        16,
    )
    return (new_errors, p_hat, q_mean)


def solution(mesh):
    cuts, dev = mesh.shape["cuts"], mesh.shape["dev"]
    cores = 2
    chips = dev // cores
    fine = Mesh(mesh.devices.reshape(cuts, chips, cores), ("cuts", "chip", "core"))
    every = ("cuts", "chip", "core")
    in_specs = (P(every, None), P(every, None), P(every, None, None), P())
    out_specs = (P(every, None, None), P(), P())
    return jax.shard_map(
        functools.partial(body, (cores, chips, cuts)),
        mesh=fine,
        in_specs=in_specs,
        out_specs=out_specs,
        check_vma=False,
    )
```

```python
import functools

import jax
import jax.numpy as jnp
from jax import lax
from jax.experimental import pallas as pl
from jax.experimental.pallas import tpu as pltpu
from jax.sharding import Mesh, PartitionSpec as P

HI = lax.Precision.HIGHEST
F32 = jnp.float32
BF16 = jnp.bfloat16
LANES = 128
VM = pl.BlockSpec(memory_space=pltpu.VMEM)
HBM = pl.BlockSpec(memory_space=pltpu.HBM)
SM = pl.BlockSpec(memory_space=pltpu.SMEM)
NN = (((1,), (0,)), ((), ()))
NT = (((1,), (1,)), ((), ()))
TN = (((0,), (0,)), ((), ()))


def dot(a, b, dims, precision=None):
    return lax.dot_general(a, b, dims, precision=precision, preferred_element_type=F32)


def split3(x):
    high = x.astype(BF16)
    rest = x - high.astype(F32)
    mid = rest.astype(BF16)
    low = (rest - mid.astype(F32)).astype(BF16)
    return jnp.concatenate([high, mid, low], axis=0)


def fold3(x):
    rows = x.shape[0] // 3
    return x[:rows] + x[rows : 2 * rows] + x[2 * rows :]


def call(kernel, outs, ins_specs, out_specs, scratch, args, name, flops, limit=24):
    return pl.pallas_call(
        kernel,
        out_shape=outs,
        in_specs=ins_specs,
        out_specs=out_specs,
        scratch_shapes=scratch,
        compiler_params=pltpu.CompilerParams(vmem_limit_bytes=limit * 1024 * 1024),
        cost_estimate=pl.CostEstimate(flops=flops, bytes_accessed=0, transcendentals=0),
        name=name,
    )(*args)


def vmem(shape, dtype=F32):
    return jax.ShapeDtypeStruct(shape, dtype)


def left_kernel(pieces, block, ids, x_hbm, y_hbm, e_hbm, q_hbm, keep, send, xv, yv, ev, q_ref, v3, total, sem):
    depth = x_hbm.shape[1]
    rank = q_ref.shape[0]
    steps = depth // block
    q_copy = pltpu.make_async_copy(q_hbm, q_ref, sem.at[1 + 2 * steps])
    q_copy.start()
    y_copy = pltpu.make_async_copy(y_hbm, yv, sem.at[0])
    y_copy.start()
    x_copies, e_copies = [], []
    for i in range(steps):
        cut = pl.ds(i * block, block)
        x_copies.append(pltpu.make_async_copy(x_hbm.at[:, cut], xv.at[:, cut], sem.at[1 + 2 * i]))
        e_copies.append(pltpu.make_async_copy(e_hbm.at[0, cut, :], ev.at[cut, :], sem.at[2 + 2 * i]))
        x_copies[i].start()
        e_copies[i].start()
    q_copy.wait()
    q3 = split3(q_ref[...])
    y_copy.wait()
    v3[...] = split3(fold3(dot(q3, yv[...], NT)))
    for i in range(steps):
        cut = pl.ds(i * block, block)
        x_copies[i].wait()
        e_copies[i].wait()
        part = fold3(dot(v3[...], xv[:, cut], NN) + dot(q3, ev[cut, :], NT))
        for j in range(block // LANES):
            at = (i * (block // LANES) + j) * rank
            total[at : at + rank, :] = part[:, j * LANES : (j + 1) * LANES]
    place(pieces, ids, total, (keep, send))


def place(pieces, ids, total, outs):
    cores, chips, cuts = pieces
    size = total.shape[0] // (cores * chips * cuts)
    for core in range(cores):
        for chip in range(chips):
            for cut in range(cuts):
                chunk = ((core ^ ids[0]) * chips + (chip ^ ids[1])) * cuts + (cut ^ ids[2])
                at = (chip * cuts + cut) * size
                start = pl.multiple_of(chunk * size, 8)
                outs[core][at : at + size, :] = total[pl.ds(start, size), :]


def sum_kernel(count, *refs):
    ins, outs = refs[:count], refs[count:]
    size = outs[0].shape[0]
    for k, out in enumerate(outs):
        rows = pl.ds(k * size, size)
        total = ins[0][rows, :]
        for other in ins[1:]:
            total = total + other[rows, :]
        out[...] = total


def add_up(ins, pieces, name):
    rows = ins[0].shape[0]
    shape = vmem((rows // pieces, LANES))
    return call(
        functools.partial(sum_kernel, len(ins)), [shape] * pieces, [VM] * len(ins), [VM] * pieces, [], ins, name, 10**7, 8
    )


def join_kernel(*refs):
    out = refs[-1]
    size = refs[0].shape[0]
    for k, part in enumerate(refs[:-1]):
        out[k * size : (k + 1) * size, :] = part[...]


def join(parts, name):
    if len(parts) == 1:
        return parts[0]
    shape = vmem((parts[0].shape[0] * len(parts), LANES))
    return call(join_kernel, shape, [VM] * len(parts), VM, [], parts, name, 10**7, 8)


def right_kernel(pieces, ids, *refs):
    cores, chips, cuts = pieces
    parts = refs[: cores * chips]
    xv, yv, ev, keep, send, left, p3, total = refs[cores * chips :]
    rank = p3.shape[0] // 3
    size = left.shape[0] // (cores * chips * cuts)
    for core in range(cores):
        for chip in range(chips):
            for cut in range(cuts):
                chunk = ((core ^ ids[0]) * chips + (chip ^ ids[1])) * cuts + (cut ^ ids[2])
                start = pl.multiple_of(chunk * size, 8)
                left[pl.ds(start, size), :] = parts[core * chips + chip][cut * size : (cut + 1) * size, :]
    for c in range(left.shape[0] // rank):
        p3[:, c * LANES : (c + 1) * LANES] = split3(left[c * rank : (c + 1) * rank, :])
    u3 = split3(fold3(dot(p3[...], xv[...], NT)))
    right = fold3(dot(p3[...], ev[...], NN) + dot(u3, yv[...], NN))
    for c in range(right.shape[1] // LANES):
        total[c * rank : (c + 1) * rank, :] = right[:, c * LANES : (c + 1) * LANES]
    place((cores, 1, 1), (ids[0], 0, 0), total, (keep, send))


def merge_kernel(block, xv, yv, ev, merged):
    for i in range(ev.shape[0] // block):
        cut = pl.ds(i * block, block)
        merged[cut, :] = dot(xv[:, cut], yv[...], TN) + ev[cut, :].astype(F32)


def factor_kernel(left, lower_inv, wide):
    rank = lower_inv.shape[0]
    for c in range(left.shape[0] // rank):
        wide[:, c * LANES : (c + 1) * LANES] = left[c * rank : (c + 1) * rank, :]
    gram = dot(wide[...], wide[...], NT, HI)
    row = lax.broadcasted_iota(jnp.int32, (rank, 2 * rank), 0)
    lane = lax.broadcasted_iota(jnp.int32, (rank, 2 * rank), 1)
    eye = jnp.where(lane - rank == row, 1.0, 0.0).astype(F32)
    work = jnp.where(lane < rank, jnp.concatenate([gram, gram], axis=1), eye)
    groups = [work[8 * g : 8 * g + 8, :] for g in range(rank // 8)]
    sub = lax.broadcasted_iota(jnp.int32, (8, 2 * rank), 0)
    for k in range(rank):
        g, s = divmod(k, 8)
        pivot = groups[g][s : s + 1, :]
        scaled = pivot / pivot[:, k : k + 1]
        for h in range(g, rank // 8):
            update = groups[h][:, k : k + 1] * scaled
            if h == g:
                update = jnp.where(sub > s, update, 0.0)
            groups[h] = groups[h] - update
    for g in range(rank // 8):
        diag = jnp.sum(jnp.where(lane[8 * g : 8 * g + 8] == row[8 * g : 8 * g + 8], groups[g], 0.0), axis=1, keepdims=True)
        lower_inv[8 * g : 8 * g + 8, :] = groups[g][:, rank:] / jnp.sqrt(diag)


def hat_kernel(left, lower_inv, p_hat, hat3):
    rank = lower_inv.shape[0]
    inv = lower_inv[...]
    for c in range(left.shape[0] // rank):
        block = left[c * rank : (c + 1) * rank, :]
        hat = dot(inv, block, NN, HI)
        rows = slice(c * LANES, (c + 1) * LANES)
        p_hat[:, rows] = hat
        hat = hat.T
        high = hat.astype(BF16)
        low = (hat - high.astype(F32)).astype(BF16)
        hat3[rows, :] = jnp.concatenate([high, low, high], axis=1)


def last_kernel(devices, block, ids, keep, other, lower_inv, hat, hat3, merged, new_errors, p_hat, q_mean, total, out, q_out, sem):
    copies = [pltpu.make_async_copy(hat, p_hat, sem.at[0])]
    copies[0].start()
    rank = lower_inv.shape[0]
    half = keep.shape[0]
    total[pl.ds(pl.multiple_of(ids[0] * half, 8), half), :] = keep[...]
    if other is not None:
        total[pl.ds(pl.multiple_of((1 - ids[0]) * half, 8), half), :] = other[...]
    wide = jnp.concatenate([total[c * rank : (c + 1) * rank, :] for c in range(total.shape[0] // rank)], axis=1)
    right = dot(lower_inv[...], wide, NN, HI) / devices
    high = right.astype(BF16)
    low = (right - high.astype(F32)).astype(BF16)
    q3 = jnp.concatenate([high, high, low], axis=0)
    q_out[...] = right
    copies.append(pltpu.make_async_copy(q_out, q_mean, sem.at[1]))
    copies[1].start()
    for i in range(merged.shape[0] // block):
        cut = pl.ds(i * block, block)
        out[cut, :] = (merged[cut, :] - dot(hat3[cut, :], q3, NN)).astype(BF16)
        copies.append(pltpu.make_async_copy(out.at[cut, :], new_errors.at[0, cut, :], sem.at[2 + i]))
        copies[2 + i].start()
    for copy in copies:
        copy.wait()


def exchange(parts, axis, size):
    got = [swap(parts[k], axis, size, k) for k in range(size - 1, 0, -1)]
    return [parts[0]] + got[::-1]


def swap(x, axis, size, by):
    return lax.ppermute(x, axis, [(i, i ^ by) for i in range(size)])


def body(sizes, inputs, cotangent, errors, previous_q):
    cores, chips, cuts = sizes
    tokens, depth = inputs.shape
    width, rank = previous_q.shape
    devices = cores * chips * cuts
    rows = depth * rank // LANES
    block = next(b for b in (512, 384, 256, LANES) if depth % b == 0)
    steps = depth // block
    share = rows // (cores * chips)
    scatter = cuts if share % (8 * cuts) == 0 else 1
    pieces = (cores, chips, scatter)
    ids = jnp.stack(
        [lax.axis_index("core"), lax.axis_index("chip"), lax.axis_index("cuts") if scatter > 1 else 0]
    ).astype(jnp.int32)
    half = vmem((rows // cores, LANES))
    keep, send, xv, yv, ev = call(
        functools.partial(left_kernel, pieces, block),
        [half, half, vmem((tokens, depth), BF16), vmem((tokens, width), BF16), vmem((depth, width), BF16)],
        [SM, HBM, HBM, HBM, HBM],
        [VM] * 5,
        [
            pltpu.VMEM((rank, width), F32),
            pltpu.VMEM((3 * rank, tokens), BF16),
            pltpu.VMEM((rows, LANES), F32),
            pltpu.SemaphoreType.DMA((2 + 2 * steps,)),
        ],
        (ids, inputs, cotangent, errors, previous_q.T),
        "left",
        10**9,
        46,
    )
    got = swap(send, "core", cores, 1)
    parts = add_up([keep, got], chips, "sum_core")
    got = exchange(parts, "chip", chips)
    parts = add_up(got, scatter, "sum_chip")
    if scatter > 1:
        got = exchange(parts, "cuts", cuts)
        mine = add_up(got, 1, "sum_cut")[0]
        mine = join(exchange([mine] * cuts, "cuts", cuts), "join_cut")
    else:
        mine = add_up(exchange(parts * cuts, "cuts", cuts), 1, "sum_cut")[0]
    parts = exchange([mine] * chips, "chip", chips)
    parts = parts + [swap(part, "core", cores, 1) for part in parts]

    merged = call(
        functools.partial(merge_kernel, block),
        vmem((depth, width)),
        [VM] * 3,
        VM,
        [],
        (xv, yv, ev),
        "merge",
        2 * tokens * depth * width,
        8,
    )
    half = vmem((width * rank // LANES // cores, LANES))
    keep, send, left = call(
        functools.partial(right_kernel, pieces),
        [half, half, vmem((rows, LANES))],
        [SM] + [VM] * (len(parts) + 3),
        [VM] * 3,
        [pltpu.VMEM((3 * rank, depth), BF16), pltpu.VMEM((width * rank // LANES, LANES), F32)],
        (ids, *parts, xv, yv, ev),
        "right",
        10**9,
        16,
    )
    got = swap(send, "core", cores, 1)
    part = add_up([keep, got], 1, "sum_core")[0]
    part = add_up(exchange([part] * chips, "chip", chips), 1, "sum_chip")[0]
    part = add_up(exchange([part] * cuts, "cuts", cuts), 1, "sum_cut")[0]
    other = swap(part, "core", cores, 1)

    lower_inv = call(
        factor_kernel, vmem((rank, rank)), [VM], VM, [pltpu.VMEM((rank, depth), F32)], (left,), "factor", 10**9, 8
    )
    hat, hat3 = call(
        hat_kernel,
        [vmem((rank, depth)), vmem((depth, 3 * rank), BF16)],
        [VM, VM],
        [VM, VM],
        [],
        (left, lower_inv),
        "hat",
        10**9,
        8,
    )
    new_errors, p_hat, q_mean = call(
        functools.partial(last_kernel, devices, block),
        [vmem((1, depth, width), BF16), vmem((rank, depth)), vmem((rank, width))],
        [SM] + [VM] * 6,
        [HBM] * 3,
        [
            pltpu.VMEM((width * rank // LANES, LANES), F32),
            pltpu.VMEM((depth, width), BF16),
            pltpu.VMEM((rank, width), F32),
            pltpu.SemaphoreType.DMA((2 + steps,)),
        ],
        (ids, part, other, lower_inv, hat, hat3, merged),
        "last",
        10**9,
        16,
    )
    return (new_errors, p_hat.T, q_mean.T)


def solution(mesh):
    cuts, dev = mesh.shape["cuts"], mesh.shape["dev"]
    cores = 2
    chips = dev // cores
    fine = Mesh(mesh.devices.reshape(cuts, chips, cores), ("cuts", "chip", "core"))
    every = ("cuts", "chip", "core")
    in_specs = (P(every, None), P(every, None), P(every, None, None), P())
    out_specs = (P(every, None, None), P(), P())
    return jax.shard_map(
        functools.partial(body, (cores, chips, cuts)),
        mesh=fine,
        in_specs=in_specs,
        out_specs=out_specs,
        check_vma=False,
    )
```

```python
import functools

import jax
import jax.numpy as jnp
from jax import lax
from jax.experimental import pallas as pl
from jax.experimental.pallas import tpu as pltpu
from jax.sharding import Mesh, PartitionSpec as P


F32 = jnp.float32
BF16 = jnp.bfloat16
LANES = 128
VM = pl.BlockSpec(memory_space=pltpu.VMEM)
HBM = pl.BlockSpec(memory_space=pltpu.HBM)
SM = pl.BlockSpec(memory_space=pltpu.SMEM)
NN = (((1,), (0,)), ((), ()))
NT = (((1,), (1,)), ((), ()))
TN = (((0,), (0,)), ((), ()))


def dot(a, b, dims, precision=None):
    return lax.dot_general(a, b, dims, precision=precision, preferred_element_type=F32)


def split3(x):
    high = x.astype(BF16)
    rest = x - high.astype(F32)
    mid = rest.astype(BF16)
    low = (rest - mid.astype(F32)).astype(BF16)
    return jnp.concatenate([high, mid, low], axis=0)


def fold3(x):
    rows = x.shape[0] // 3
    return x[:rows] + x[rows : 2 * rows] + x[2 * rows :]


def call(kernel, outs, ins_specs, out_specs, scratch, args, flops, limit=24):
    return pl.pallas_call(
        kernel,
        out_shape=outs,
        in_specs=ins_specs,
        out_specs=out_specs,
        scratch_shapes=scratch,
        compiler_params=pltpu.CompilerParams(vmem_limit_bytes=limit * 1024 * 1024),
        cost_estimate=pl.CostEstimate(flops=flops, bytes_accessed=0, transcendentals=0),
    )(*args)


def vmem(shape, dtype=F32):
    return jax.ShapeDtypeStruct(shape, dtype)


def left_half(total, block, start, xv, ev, v3, q3, ready=None):
    rank = v3.shape[0] // 3
    for i in range(total.shape[0] // rank * LANES // block):
        if ready is not None:
            ready(i)
        cut = pl.ds(pl.multiple_of(start + i * block, LANES), block)
        part = fold3(dot(v3[...], xv[:, cut], NN) + dot(q3[...], ev[cut, :], NT))
        for j in range(block // LANES):
            at = (i * (block // LANES) + j) * rank
            total[at : at + rank, :] = part[:, j * LANES : (j + 1) * LANES]


def put_chips(chips, ids, total, out):
    size = out.shape[0] // chips
    for chip in range(chips):
        start = pl.multiple_of((chip ^ ids[1]) * size, 8)
        out[chip * size : (chip + 1) * size, :] = total[pl.ds(start, size), :]


def first_kernel(cores, chips, block, ids, x_hbm, y_hbm, e_hbm, q_hbm, send, xv, yv, ev, v3, q3, q_ref, total, sem):
    depth = x_hbm.shape[1]
    half = depth // cores
    steps = half // block
    q_copy = pltpu.make_async_copy(q_hbm, q_ref, sem.at[0])
    y_copy = pltpu.make_async_copy(y_hbm, yv, sem.at[1])
    q_copy.start()
    y_copy.start()
    copies = []
    for k in range(cores):
        start = ((ids[0] + 1 + k) % cores) * half
        for i in range(steps):
            cut = pl.ds(pl.multiple_of(start + i * block, LANES), block)
            at = 2 + 2 * (k * steps + i)
            pair = (
                pltpu.make_async_copy(x_hbm.at[:, cut], xv.at[:, cut], sem.at[at]),
                pltpu.make_async_copy(e_hbm.at[0, cut, :], ev.at[cut, :], sem.at[at + 1]),
            )
            pair[0].start()
            pair[1].start()
            copies.append(pair)

    def ready(i):
        copies[i][0].wait()
        copies[i][1].wait()

    q_copy.wait()
    q3[...] = split3(q_ref[...])
    y_copy.wait()
    v3[...] = split3(fold3(dot(q3[...], yv[...], NT)))
    left_half(total, block, ((ids[0] + 1) % cores) * half, xv, ev, v3, q3, ready)
    put_chips(chips, ids, total, send)
    for i in range(steps, cores * steps):
        ready(i)


def second_kernel(chips, block, ids, xv, ev, v3, q3, keep, total):
    left_half(total, block, ids[0] * (total.shape[0] // (v3.shape[0] // 3) * LANES), xv, ev, v3, q3)
    put_chips(chips, ids, total, keep)


def sum_kernel(count, *refs):
    ins, outs = refs[:count], refs[count:]
    size = outs[0].shape[0]
    for k, out in enumerate(outs):
        rows = pl.ds(k * size, size)
        total = ins[0][rows, :]
        for other in ins[1:]:
            total = total + other[rows, :]
        out[...] = total


def add_up(ins, pieces):
    rows = ins[0].shape[0]
    shape = vmem((rows // pieces, LANES))
    return call(
        functools.partial(sum_kernel, len(ins)), [shape] * pieces, [VM] * len(ins), [VM] * pieces, [], ins, 10**7, 8
    )


def merge_kernel(span, xv, yv, ev, merged, parts):
    for i in range(ev.shape[0] // span):
        cut = slice(i * span, (i + 1) * span)
        block = dot(xv[:, cut], yv[...], TN) + ev[cut, :].astype(F32)
        merged[cut, :] = block
        high = block.astype(BF16)
        parts[2 * i * span : (2 * i + 1) * span, :] = high
        parts[(2 * i + 1) * span : (2 * i + 2) * span, :] = (block - high.astype(F32)).astype(BF16)


def chunk_of(chips, ids, where):
    return (where[0] ^ ids[0]) * chips + (where[1] ^ ids[1])


def chunk_kernel(chips, places, first, last, ids, *refs):
    parts, rest = refs[: len(places)], refs[len(places) :]
    merged2, rest = rest[0], rest[1:]
    before, rest = (None, rest) if first else (rest[0], rest[1:])
    p3 = rest[0]
    rank = p3.shape[0] // 3
    span = parts[0].shape[0] // rank * LANES
    t = None if first else before[...]
    for i, (part, where) in enumerate(zip(parts, places)):
        for c in range(span // LANES):
            at = i * span + c * LANES
            p3[:, at : at + LANES] = split3(part[c * rank : (c + 1) * rank, :])
        rows = pl.ds(pl.multiple_of(chunk_of(chips, ids, where) * (2 * span), 16), 2 * span)
        mine = p3[:, i * span : (i + 1) * span]
        new = dot(jnp.concatenate([mine, mine], axis=1), merged2[rows, :], NN)
        t = new if t is None else t + new
    if not last:
        rest[1][...] = t
        return
    keep, send, total = rest[1:]
    right = fold3(t)
    for c in range(right.shape[1] // LANES):
        total[c * rank : (c + 1) * rank, :] = right[:, c * LANES : (c + 1) * LANES]
    size = keep.shape[0]
    keep[...] = total[pl.ds(pl.multiple_of(ids[0] * size, 8), size), :]
    send[...] = total[pl.ds(pl.multiple_of((1 - ids[0]) * size, 8), size), :]


def gram_kernel(*refs):
    gram = refs[-1]
    rank = gram.shape[0]
    full = sum(dot(p3[...], p3[...], NT) for p3 in refs[:-1])
    full = fold3(full)
    gram[...] = full[:, :rank] + full[:, rank : 2 * rank] + full[:, 2 * rank :]


def factor_kernel(gram, lower_inv):
    rank = gram.shape[0]
    n = 8
    row = lax.broadcasted_iota(jnp.int32, (rank, rank), 0)
    lane = lax.broadcasted_iota(jnp.int32, (rank, rank), 1)
    eye = jnp.where(lane == row, 1.0, 0.0).astype(F32)
    work = jnp.concatenate([eye, gram[...]], axis=1)
    groups = [work[n * g : n * g + n, :] for g in range(rank // n)]
    wide = (n, 2 * rank)

    def column(x, k):
        return jnp.broadcast_to(x[:, rank + k : rank + k + 1], wide)

    def line(x, i):
        return jnp.broadcast_to(x[i : i + 1, :], wide)

    sub = lax.broadcasted_iota(jnp.int32, wide, 0)
    for g in range(rank // n):
        base = n * g
        cols = [column(groups[g], base + j) for j in range(n)]
        b = {(i, j): line(cols[j], i) for j in range(n) for i in range(j, n)}
        low, inv = {}, []
        for s in range(n):
            inv.append(1.0 / b[s, s])
            for i in range(s + 1, n):
                low[i, s] = b[i, s] * inv[s]
            for j in range(s + 1, n):
                for i in range(j, n):
                    b[i, j] = b[i, j] - low[i, s] * b[j, s]
        rows = []
        for i in range(n):
            r = line(groups[g], i)
            for s in range(i):
                r = r - low[i, s] * rows[s]
            rows.append(r)
        for h in range(g + 1, rank // n):
            x = [column(groups[h], base + s) for s in range(n)]
            for s in range(n):
                for t in range(s):
                    x[s] = x[s] - low[s, t] * x[t]
            new = groups[h]
            for s in range(n):
                new = new - (x[s] * inv[s]) * rows[s]
            groups[h] = new
        out = jnp.zeros(wide, F32)
        for i in range(n):
            out = jnp.where(sub == i, rows[i] * jnp.sqrt(inv[i]), out)
        lower_inv[base : base + n, :] = out[:, :rank]


def hat_kernel(cores, chips, places, ids, *refs):
    p3s, (lower_inv, p_hat, hat3) = refs[:-3], refs[-3:]
    rank = lower_inv.shape[0]
    inv3 = split3(lower_inv[...])
    at = 0
    for p3 in p3s:
        full = dot(inv3, p3[:rank, :], NN)
        mids = dot(inv3[: 2 * rank], p3[rank : 2 * rank, :], NN)
        hats = fold3(full) + (mids[:rank] + mids[rank:]) + dot(inv3[:rank], p3[2 * rank :, :], NN)
        span = p_hat.shape[1] // (cores * chips)
        for i in range(p3.shape[1] // span):
            start = chunk_of(chips, ids, places[at]) * span
            at += 1
            hat = hats[:, i * span : (i + 1) * span]
            p_hat[:, pl.ds(pl.multiple_of(start, LANES), span)] = hat
            for c in range(span // LANES):
                turned = hat[:, c * LANES : (c + 1) * LANES].T
                high = turned.astype(BF16)
                low = (turned - high.astype(F32)).astype(BF16)
                rows = pl.ds(pl.multiple_of(start + c * LANES, LANES), LANES)
                hat3[rows, :] = jnp.concatenate([high, low, high], axis=1)


def last_kernel(devices, block, ids, keep, other, lower_inv, hat, hat3, merged, new_errors, p_hat, q_mean, total, out, q_out, sem):
    copies = [pltpu.make_async_copy(hat, p_hat, sem.at[0])]
    copies[0].start()
    rank = lower_inv.shape[0]
    half = keep.shape[0]
    total[pl.ds(pl.multiple_of(ids[0] * half, 8), half), :] = keep[...]
    if other is not None:
        total[pl.ds(pl.multiple_of((1 - ids[0]) * half, 8), half), :] = other[...]
    wide = jnp.concatenate([total[c * rank : (c + 1) * rank, :] for c in range(total.shape[0] // rank)], axis=1)
    a, b = split3(lower_inv[...]), split3(wide)
    ah, am, al = a[:rank], a[rank : 2 * rank], a[2 * rank :]
    bh, bm, bl = b[:rank], b[rank : 2 * rank], b[2 * rank :]
    right = dot(jnp.concatenate([ah, ah, am, ah, al, am], axis=1), jnp.concatenate([bh, bm, bh, bl, bh, bm], axis=0), NN)
    right = right / devices
    high = right.astype(BF16)
    low = (right - high.astype(F32)).astype(BF16)
    q3 = jnp.concatenate([high, high, low], axis=0)
    q_out[...] = right
    copies.append(pltpu.make_async_copy(q_out, q_mean, sem.at[1]))
    copies[1].start()
    for i in range(merged.shape[0] // block):
        cut = pl.ds(i * block, block)
        out[cut, :] = (merged[cut, :] - dot(hat3[cut, :], q3, NN)).astype(BF16)
        copies.append(pltpu.make_async_copy(out.at[cut, :], new_errors.at[0, cut, :], sem.at[2 + i]))
        copies[2 + i].start()
    for copy in copies:
        copy.wait()


def exchange(parts, axis, size):
    return [parts[0]] + [swap(parts[k], axis, size, k) for k in range(1, size)]


def swap(x, axis, size, by):
    return lax.ppermute(x, axis, [(i, i ^ by) for i in range(size)])


def body(sizes, *args):
    return step(sizes, *args)


def step(sizes, inputs, cotangent, errors, previous_q):
    cores, chips, groups, cuts = sizes
    tokens, depth = inputs.shape
    width, rank = previous_q.shape
    devices = cores * chips * groups * cuts
    rows = depth * rank // LANES
    span = depth // (cores * chips)
    block = next(b for b in (512, 384, 256, LANES) if depth // cores % b == 0)
    steps = depth // block
    ids = jnp.stack([lax.axis_index("core"), lax.axis_index("chip")]).astype(jnp.int32)
    half = vmem((rows // cores, LANES))
    total = pltpu.VMEM((rows // cores, LANES), F32)
    send, xv, yv, ev, v3, q3 = call(
        functools.partial(first_kernel, cores, chips, block),
        [
            half,
            vmem((tokens, depth), BF16),
            vmem((tokens, width), BF16),
            vmem((depth, width), BF16),
            vmem((3 * rank, tokens), BF16),
            vmem((3 * rank, width), BF16),
        ],
        [SM] + [HBM] * 4,
        [VM] * 6,
        [pltpu.VMEM((rank, width), F32), total, pltpu.SemaphoreType.DMA((2 + 2 * steps,))],
        (ids, inputs, cotangent, errors, previous_q.T),
        10**9,
        46,
    )
    got = swap(send, "core", cores, 1)
    keep = call(
        functools.partial(second_kernel, chips, block),
        half,
        [SM] + [VM] * 4,
        VM,
        [total],
        (ids, xv, ev, v3, q3),
        10**9,
        8,
    )
    parts = add_up([keep, got], chips)
    parts = add_up(exchange(parts, "chip", chips), 1)
    if groups > 1:
        parts = add_up(exchange(parts * groups, "group", groups), 1)
    parts = add_up(exchange(parts * cuts, "cuts", cuts), 1)
    parts = exchange(parts * chips, "chip", chips)
    parts = parts + [swap(part, "core", cores, 1) for part in parts]

    merged, merged2 = call(
        functools.partial(merge_kernel, span),
        [vmem((depth, width)), vmem((2 * depth, width), BF16)],
        [VM] * 3,
        [VM] * 2,
        [],
        (xv, yv, ev),
        10**9,
        8,
    )
    places = [(core, chip) for core in range(cores) for chip in range(chips)]
    batches = [[0, chips], list(range(1, chips)), list(range(chips + 1, 2 * chips))]
    share = vmem((width * rank // LANES // cores, LANES))
    sums, p3s, order = [], [], []
    for at, batch in enumerate(batches):
        end = at == len(batches) - 1
        p3, *sums = call(
            functools.partial(chunk_kernel, chips, [places[k] for k in batch], at == 0, end),
            [vmem((3 * rank, span * len(batch)), BF16)] + ([share, share] if end else [vmem((3 * rank, width))]),
            [SM] + [VM] * (len(batch) + 1 + len(sums)),
            [VM] * (3 if end else 2),
            [pltpu.VMEM((width * rank // LANES, LANES), F32)] if end else [],
            (ids, *[parts[k] for k in batch], merged2, *sums),
            10**8,
            8,
        )
        p3s.append(p3)
        order += [places[k] for k in batch]
    keep, send = sums
    got = swap(send, "core", cores, 1)
    part = add_up([keep, got], 1)[0]
    part = add_up(exchange([part] * chips, "chip", chips), 1)[0]
    if groups > 1:
        part = add_up(exchange([part] * groups, "group", groups), 1)[0]
    part = add_up(exchange([part] * cuts, "cuts", cuts), 1)[0]
    other = swap(part, "core", cores, 1)

    gram = call(gram_kernel, vmem((rank, rank)), [VM] * len(p3s), VM, [], p3s, 10**8, 8)
    lower_inv = call(factor_kernel, vmem((rank, rank)), [VM], VM, [], (gram,), 10**9, 8)
    hat, hat3 = call(
        functools.partial(hat_kernel, cores, chips, order),
        [vmem((rank, depth)), vmem((depth, 3 * rank), BF16)],
        [SM] + [VM] * (len(p3s) + 1),
        [VM, VM],
        [],
        (ids, *p3s, lower_inv),
        10**9,
        8,
    )
    new_errors, p_hat, q_mean = call(
        functools.partial(last_kernel, devices, block),
        [vmem((1, depth, width), BF16), vmem((rank, depth)), vmem((rank, width))],
        [SM] + [VM] * 6,
        [HBM] * 3,
        [
            pltpu.VMEM((width * rank // LANES, LANES), F32),
            pltpu.VMEM((depth, width), BF16),
            pltpu.VMEM((rank, width), F32),
            pltpu.SemaphoreType.DMA((2 + steps,)),
        ],
        (ids, part, other, lower_inv, hat, hat3, merged),
        10**9,
        16,
    )
    return (new_errors, p_hat.T, q_mean.T)


def solution(mesh):
    cuts, dev = mesh.shape["cuts"], mesh.shape["dev"]
    cores = 2
    every = ("cuts", "group", "chip", "core")

    def program(inputs, cotangent, errors, previous_q):
        columns = inputs.shape[1] // (cores * LANES)
        chips = next(n for n in range(dev // cores, 0, -1) if dev // cores % n == 0 and columns % n == 0)
        groups = dev // (cores * chips)
        fine = Mesh(mesh.devices.reshape(cuts, groups, chips, cores), every)
        run = jax.shard_map(
            functools.partial(body, (cores, chips, groups, cuts)),
            mesh=fine,
            in_specs=(P(every, None), P(every, None), P(every, None, None), P()),
            out_specs=(P(every, None, None), P(), P()),
            check_vma=False,
        )
        return run(inputs, cotangent, errors, previous_q)

    return program
```

```python
import functools

import jax
import jax.numpy as jnp
from jax import lax
from jax.experimental import pallas as pl
from jax.experimental.pallas import tpu as pltpu
from jax.sharding import Mesh, PartitionSpec as P


F32 = jnp.float32
BF16 = jnp.bfloat16
LANES = 128
VM = pl.BlockSpec(memory_space=pltpu.VMEM)
HBM = pl.BlockSpec(memory_space=pltpu.HBM)
SM = pl.BlockSpec(memory_space=pltpu.SMEM)
NN = (((1,), (0,)), ((), ()))
NT = (((1,), (1,)), ((), ()))
TN = (((0,), (0,)), ((), ()))


def dot(a, b, dims, precision=None):
    return lax.dot_general(a, b, dims, precision=precision, preferred_element_type=F32)


def split3(x):
    high = x.astype(BF16)
    rest = x - high.astype(F32)
    mid = rest.astype(BF16)
    low = (rest - mid.astype(F32)).astype(BF16)
    return jnp.concatenate([high, mid, low], axis=0)


def fold3(x):
    rows = x.shape[0] // 3
    return x[:rows] + x[rows : 2 * rows] + x[2 * rows :]


def call(kernel, outs, ins_specs, out_specs, scratch, args, flops, limit, aliases={}):
    return pl.pallas_call(
        kernel,
        out_shape=outs,
        in_specs=ins_specs,
        out_specs=out_specs,
        scratch_shapes=scratch,
        compiler_params=pltpu.CompilerParams(vmem_limit_bytes=limit * 1024 * 1024),
        cost_estimate=pl.CostEstimate(flops=flops, bytes_accessed=0, transcendentals=0),
        input_output_aliases=aliases,
    )(*args)


def vmem(shape, dtype=F32):
    return jax.ShapeDtypeStruct(shape, dtype)


def left_half(total, block, start, xv, ev, v3, q3):
    rank = v3.shape[0] // 3
    for i in range(total.shape[0] // rank * LANES // block):
        cut = pl.ds(pl.multiple_of(start + i * block, LANES), block)
        part = fold3(dot(v3[...], xv[:, cut], NN) + dot(q3[...], ev[cut, :], NT))
        for j in range(block // LANES):
            at = (i * (block // LANES) + j) * rank
            total[at : at + rank, :] = part[:, j * LANES : (j + 1) * LANES]


def put_chips(chips, ids, total, out):
    size = out.shape[0] // chips
    for chip in range(chips):
        start = pl.multiple_of((chip ^ ids[1]) * size, 8)
        out[chip * size : (chip + 1) * size, :] = total[pl.ds(start, size), :]


def cuts_of(block, start, half):
    return [pl.ds(pl.multiple_of(start + i * block, LANES), block) for i in range(half // block)]


def load_kernel(cores, block, ids, e_hbm, ev, sem):
    half = ev.shape[0] // cores
    cut = cuts_of(block, (1 - ids[0]) * half, half)[0]
    copy = pltpu.make_async_copy(e_hbm.at[0, cut, :], ev.at[cut, :], sem)
    copy.start()
    copy.wait()


def first_kernel(cores, chips, block, ids, x_hbm, e_hbm, y, q, e_in, send, xv, ev, v3, q3, total, sem):
    half = xv.shape[1] // cores
    theirs, own = cuts_of(block, (1 - ids[0]) * half, half), cuts_of(block, ids[0] * half, half)
    count = len(own)
    x_copies, e_copies = [], []
    for i, cut in enumerate(theirs + own):
        x_copies.append(pltpu.make_async_copy(x_hbm.at[:, cut], xv.at[:, cut], sem.at[2 * i]))
        if i > 0:
            e_copies.append(pltpu.make_async_copy(e_hbm.at[0, cut, :], ev.at[cut, :], sem.at[2 * i + 1]))
    for copy in e_copies[: count - 1] + x_copies + e_copies[count - 1 :]:
        copy.start()
    q3[...] = split3(q[...])
    rank = q.shape[0]
    tiles = block // LANES
    for i, cut in enumerate(theirs):
        if i > 0:
            e_copies[i - 1].wait()
        part = fold3(dot(q3[...], (e_in if i == 0 else ev)[cut, :], NT))
        for j in range(tiles):
            at = (i * tiles + j) * rank
            total[at : at + rank, :] = part[:, j * LANES : (j + 1) * LANES]
        if i == 0:
            v3[...] = split3(fold3(dot(q3[...], y[...], NT)))
    for i, cut in enumerate(theirs):
        x_copies[i].wait()
        part = fold3(dot(v3[...], xv[:, cut], NN))
        for j in range(tiles):
            at = (i * tiles + j) * rank
            total[at : at + rank, :] += part[:, j * LANES : (j + 1) * LANES]
    put_chips(chips, ids, total, send)
    for copy in x_copies[count:] + e_copies[count - 1 :]:
        copy.wait()


def second_kernel(chips, block, ids, xv, ev, v3, q3, keep, total):
    left_half(total, block, ids[0] * (total.shape[0] // (v3.shape[0] // 3) * LANES), xv, ev, v3, q3)
    put_chips(chips, ids, total, keep)


def sum_kernel(count, *refs):
    ins, outs = refs[:count], refs[count:]
    size = outs[0].shape[0]
    for k, out in enumerate(outs):
        rows = pl.ds(k * size, size)
        total = ins[0][rows, :]
        for other in ins[1:]:
            total = total + other[rows, :]
        out[...] = total


def add_up(ins, pieces):
    rows = ins[0].shape[0]
    shape = vmem((rows // pieces, LANES))
    return call(
        functools.partial(sum_kernel, len(ins)), [shape] * pieces, [VM] * len(ins), [VM] * pieces, [], ins, 10**7, 8
    )


def merge_kernel(span, xv, yv, ev, merged, parts):
    for i in range(ev.shape[0] // span):
        cut = slice(i * span, (i + 1) * span)
        block = dot(xv[:, cut], yv[...], TN) + ev[cut, :].astype(F32)
        merged[cut, :] = block
        high = block.astype(BF16)
        parts[2 * i * span : (2 * i + 1) * span, :] = high
        parts[(2 * i + 1) * span : (2 * i + 2) * span, :] = (block - high.astype(F32)).astype(BF16)


def chunk_of(chips, ids, where):
    return (where[0] ^ ids[0]) * chips + (where[1] ^ ids[1])


def chunk_kernel(chips, places, first, last, ids, *refs):
    parts, rest = refs[: len(places)], refs[len(places) :]
    merged2, rest = rest[0], rest[1:]
    before, rest = (None, rest) if first else (rest[0], rest[1:])
    p3 = rest[0]
    rank = p3.shape[0] // 3
    span = parts[0].shape[0] // rank * LANES
    t = None if first else before[...]
    for i, (part, where) in enumerate(zip(parts, places)):
        for c in range(span // LANES):
            at = i * span + c * LANES
            p3[:, at : at + LANES] = split3(part[c * rank : (c + 1) * rank, :])
        rows = pl.ds(pl.multiple_of(chunk_of(chips, ids, where) * (2 * span), 16), 2 * span)
        mine = p3[:, i * span : (i + 1) * span]
        new = dot(jnp.concatenate([mine, mine], axis=1), merged2[rows, :], NN)
        t = new if t is None else t + new
    if not last:
        rest[1][...] = t
        return
    keep, send, total = rest[1:]
    right = fold3(t)
    for c in range(right.shape[1] // LANES):
        total[c * rank : (c + 1) * rank, :] = right[:, c * LANES : (c + 1) * LANES]
    size = keep.shape[0]
    keep[...] = total[pl.ds(pl.multiple_of(ids[0] * size, 8), size), :]
    send[...] = total[pl.ds(pl.multiple_of((1 - ids[0]) * size, 8), size), :]


def gram_kernel(*refs):
    gram = refs[-1]
    rank = gram.shape[0]
    full = sum(dot(p3[...], p3[...], NT) for p3 in refs[:-1])
    full = fold3(full)
    gram[...] = full[:, :rank] + full[:, rank : 2 * rank] + full[:, 2 * rank :]


def factor_kernel(gram, lower_inv):
    rank = gram.shape[0]
    n = 8
    row = lax.broadcasted_iota(jnp.int32, (rank, rank), 0)
    lane = lax.broadcasted_iota(jnp.int32, (rank, rank), 1)
    eye = jnp.where(lane == row, 1.0, 0.0).astype(F32)
    work = jnp.concatenate([eye, gram[...]], axis=1)
    groups = [work[n * g : n * g + n, :] for g in range(rank // n)]
    wide = (n, 2 * rank)
    def column(x, k):
        return jnp.broadcast_to(x[:, rank + k : rank + k + 1], wide)
    def line(x, i):
        return jnp.broadcast_to(x[i : i + 1, :], wide)
    sub = lax.broadcasted_iota(jnp.int32, wide, 0)
    for g in range(rank // n):
        base = n * g
        cols = [column(groups[g], base + j) for j in range(n)]
        b = {(i, j): line(cols[j], i) for j in range(n) for i in range(j, n)}
        low, inv = {}, []
        for s in range(n):
            inv.append(1.0 / b[s, s])
            for i in range(s + 1, n):
                low[i, s] = b[i, s] * inv[s]
            for j in range(s + 1, n):
                for i in range(j, n):
                    b[i, j] = b[i, j] - low[i, s] * b[j, s]
        rows = []
        for i in range(n):
            r = line(groups[g], i)
            for s in range(i):
                r = r - low[i, s] * rows[s]
            rows.append(r)
        for h in range(g + 1, rank // n):
            x = [column(groups[h], base + s) for s in range(n)]
            for s in range(n):
                for t in range(s):
                    x[s] = x[s] - low[s, t] * x[t]
            new = groups[h]
            for s in range(n):
                new = new - (x[s] * inv[s]) * rows[s]
            groups[h] = new
        out = jnp.zeros(wide, F32)
        for i in range(n):
            out = jnp.where(sub == i, rows[i] * jnp.sqrt(inv[i]), out)
        lower_inv[base : base + n, :] = out[:, :rank]


def hat_kernel(cores, chips, places, ids, *refs):
    p3s, (lower_inv, out, hat3, p_hat, sem) = refs[:-5], refs[-5:]
    rank = lower_inv.shape[0]
    inv3 = split3(lower_inv[...])
    at = 0
    for p3 in p3s:
        full = dot(inv3, p3[:rank, :], NN)
        mids = dot(inv3[: 2 * rank], p3[rank : 2 * rank, :], NN)
        hats = fold3(full) + (mids[:rank] + mids[rank:]) + dot(inv3[:rank], p3[2 * rank :, :], NN)
        span = p_hat.shape[1] // (cores * chips)
        for i in range(p3.shape[1] // span):
            start = chunk_of(chips, ids, places[at]) * span
            at += 1
            hat = hats[:, i * span : (i + 1) * span]
            p_hat[:, pl.ds(pl.multiple_of(start, LANES), span)] = hat
            for c in range(span // LANES):
                turned = hat[:, c * LANES : (c + 1) * LANES].T
                high = turned.astype(BF16)
                low = (turned - high.astype(F32)).astype(BF16)
                rows = pl.ds(pl.multiple_of(start + c * LANES, LANES), LANES)
                hat3[rows, :] = jnp.concatenate([high, low, high], axis=1)
    copy = pltpu.make_async_copy(p_hat, out, sem)
    copy.start()
    copy.wait()


def last_kernel(devices, block, ids, keep, other, lower_inv, hat3, merged, new_errors, q_mean, total, out, q_out, sem):
    rank = lower_inv.shape[0]
    half = keep.shape[0]
    total[pl.ds(pl.multiple_of(ids[0] * half, 8), half), :] = keep[...]
    if other is not None:
        total[pl.ds(pl.multiple_of((1 - ids[0]) * half, 8), half), :] = other[...]
    wide = jnp.concatenate([total[c * rank : (c + 1) * rank, :] for c in range(total.shape[0] // rank)], axis=1)
    a, b = split3(lower_inv[...]), split3(wide)
    ah, am, al = a[:rank], a[rank : 2 * rank], a[2 * rank :]
    bh, bm, bl = b[:rank], b[rank : 2 * rank], b[2 * rank :]
    right = dot(jnp.concatenate([ah, ah, am, ah, al, am], axis=1), jnp.concatenate([bh, bm, bh, bl, bh, bm], axis=0), NN)
    right = right / devices
    high = right.astype(BF16)
    low = (right - high.astype(F32)).astype(BF16)
    q3 = jnp.concatenate([high, high, low], axis=0)
    q_out[...] = right
    copies = [pltpu.make_async_copy(q_out, q_mean, sem.at[0])]
    copies[0].start()
    for i in range(merged.shape[0] // block):
        cut = pl.ds(i * block, block)
        out[cut, :] = (merged[cut, :] - dot(hat3[cut, :], q3, NN)).astype(BF16)
        copies.append(pltpu.make_async_copy(out.at[cut, :], new_errors.at[0, cut, :], sem.at[1 + i]))
        copies[1 + i].start()
    for copy in copies:
        copy.wait()


def exchange(parts, axis, size):
    return [parts[0]] + [swap(parts[k], axis, size, k) for k in range(1, size)]


def swap(x, axis, size, by):
    return lax.ppermute(x, axis, [(i, i ^ by) for i in range(size)])


def body(sizes, *args):
    return step(sizes, *args)


def step(sizes, inputs, cotangent, errors, previous_q):
    cores, chips, groups, cuts = sizes
    tokens, depth = inputs.shape
    width, rank = previous_q.shape
    devices = cores * chips * groups * cuts
    rows = depth * rank // LANES
    span = depth // (cores * chips)
    block = next(b for b in (512, 384, 256, LANES) if depth // cores % b == 0)
    tail = block // 2
    ids = jnp.stack([lax.axis_index("core"), lax.axis_index("chip")]).astype(jnp.int32)
    half = vmem((rows // cores, LANES))
    total = pltpu.VMEM((rows // cores, LANES), F32)
    held = vmem((depth, width), BF16)
    blocks = depth // cores // block
    ev = call(
        functools.partial(load_kernel, cores, block),
        held,
        [SM, HBM],
        VM,
        [pltpu.SemaphoreType.DMA],
        (ids, errors),
        10**9,
        49,
    )
    send, xv, ev, v3, q3 = call(
        functools.partial(first_kernel, cores, chips, block),
        [half, vmem((tokens, depth), BF16), held, vmem((3 * rank, tokens), BF16), vmem((3 * rank, width), BF16)],
        [SM, HBM, HBM] + [VM] * 3,
        [VM] * 5,
        [total, pltpu.SemaphoreType.DMA((4 * blocks,))],
        (ids, inputs, errors, cotangent, previous_q.T, ev),
        10**9,
        46,
        {5: 2},
    )
    got = swap(send, "core", cores, 1)
    keep = call(
        functools.partial(second_kernel, chips, block),
        half,
        [SM] + [VM] * 4,
        VM,
        [total],
        (ids, xv, ev, v3, q3),
        10**9,
        8,
    )
    parts = add_up([keep, got], chips)
    parts = add_up(exchange(parts, "chip", chips), 1)
    if groups > 1:
        parts = add_up(exchange(parts * groups, "group", groups), 1)
    parts = add_up(exchange(parts * cuts, "cuts", cuts), 1)
    parts = exchange(parts * chips, "chip", chips)
    parts = parts + [swap(part, "core", cores, 1) for part in parts]

    merged, merged2 = call(
        functools.partial(merge_kernel, span),
        [vmem((depth, width)), vmem((2 * depth, width), BF16)],
        [VM] * 3,
        [VM] * 2,
        [],
        (xv, cotangent, ev),
        10**9,
        8,
    )
    places = [(core, chip) for core in range(cores) for chip in range(chips)]
    batches = [[0], [chips, *range(1, chips)], list(range(chips + 1, 2 * chips))]
    share = vmem((width * rank // LANES // cores, LANES))
    sums, p3s, order = [], [], []
    for at, batch in enumerate(batches):
        end = at == len(batches) - 1
        p3, *sums = call(
            functools.partial(chunk_kernel, chips, [places[k] for k in batch], at == 0, end),
            [vmem((3 * rank, span * len(batch)), BF16)] + ([share, share] if end else [vmem((3 * rank, width))]),
            [SM] + [VM] * (len(batch) + 1 + len(sums)),
            [VM] * (3 if end else 2),
            [pltpu.VMEM((width * rank // LANES, LANES), F32)] if end else [],
            (ids, *[parts[k] for k in batch], merged2, *sums),
            10**8,
            8,
        )
        p3s.append(p3)
        order += [places[k] for k in batch]
    keep, send = sums
    got = swap(send, "core", cores, 1)
    part = add_up([keep, got], 1)[0]
    part = add_up(exchange([part] * chips, "chip", chips), 1)[0]
    if groups > 1:
        part = add_up(exchange([part] * groups, "group", groups), 1)[0]
    part = add_up(exchange([part] * cuts, "cuts", cuts), 1)[0]
    other = swap(part, "core", cores, 1)

    gram = call(gram_kernel, vmem((rank, rank)), [VM] * len(p3s), VM, [], p3s, 10**8, 8)
    lower_inv = call(factor_kernel, vmem((rank, rank)), [VM], VM, [], (gram,), 10**9, 8)
    p_hat, hat3 = call(
        functools.partial(hat_kernel, cores, chips, order),
        [vmem((rank, depth)), vmem((depth, 3 * rank), BF16)],
        [SM] + [VM] * (len(p3s) + 1),
        [HBM, VM],
        [pltpu.VMEM((rank, depth), F32), pltpu.SemaphoreType.DMA],
        (ids, *p3s, lower_inv),
        10**9,
        8,
    )
    new_errors, q_mean = call(
        functools.partial(last_kernel, devices, tail),
        [vmem((1, depth, width), BF16), vmem((rank, width))],
        [SM] + [VM] * 5,
        [HBM] * 2,
        [
            pltpu.VMEM((width * rank // LANES, LANES), F32),
            pltpu.VMEM((depth, width), BF16),
            pltpu.VMEM((rank, width), F32),
            pltpu.SemaphoreType.DMA((1 + depth // tail,)),
        ],
        (ids, part, other, lower_inv, hat3, merged),
        10**9,
        16,
    )
    return (new_errors, p_hat.T, q_mean.T)


def solution(mesh):
    cuts, dev = mesh.shape["cuts"], mesh.shape["dev"]
    cores = 2
    every = ("cuts", "group", "chip", "core")

    def program(inputs, cotangent, errors, previous_q):
        columns = inputs.shape[1] // (cores * LANES)
        chips = next(n for n in range(dev // cores, 0, -1) if dev // cores % n == 0 and columns % n == 0)
        groups = dev // (cores * chips)
        fine = Mesh(mesh.devices.reshape(cuts, groups, chips, cores), every)
        run = jax.shard_map(
            functools.partial(body, (cores, chips, groups, cuts)),
            mesh=fine,
            in_specs=(P(every, None), P(every, None), P(every, None, None), P()),
            out_specs=(P(every, None, None), P(), P()),
            check_vma=False,
        )
        return run(inputs, cotangent, errors, previous_q)

    return program
```

```python
import functools

import jax
import jax.numpy as jnp
from jax import lax
from jax.experimental import pallas as pl
from jax.experimental.pallas import tpu as pltpu
from jax.sharding import Mesh, PartitionSpec as P


F32 = jnp.float32
BF16 = jnp.bfloat16
LANES = 128
VM = pl.BlockSpec(memory_space=pltpu.VMEM)
HBM = pl.BlockSpec(memory_space=pltpu.HBM)
SM = pl.BlockSpec(memory_space=pltpu.SMEM)
NN = (((1,), (0,)), ((), ()))
NT = (((1,), (1,)), ((), ()))
TN = (((0,), (0,)), ((), ()))


def dot(a, b, dims, precision=None):
    return lax.dot_general(a, b, dims, precision=precision, preferred_element_type=F32)


def split3(x):
    high = x.astype(BF16)
    rest = x - high.astype(F32)
    mid = rest.astype(BF16)
    low = (rest - mid.astype(F32)).astype(BF16)
    return jnp.concatenate([high, mid, low], axis=0)


def fold3(x):
    rows = x.shape[0] // 3
    return x[:rows] + x[rows : 2 * rows] + x[2 * rows :]


def call(kernel, outs, ins_specs, out_specs, scratch, args, flops, limit, aliases={}):
    return pl.pallas_call(
        kernel,
        out_shape=outs,
        in_specs=ins_specs,
        out_specs=out_specs,
        scratch_shapes=scratch,
        compiler_params=pltpu.CompilerParams(vmem_limit_bytes=limit * 1024 * 1024),
        cost_estimate=pl.CostEstimate(flops=flops, bytes_accessed=0, transcendentals=0),
        input_output_aliases=aliases,
    )(*args)


def vmem(shape, dtype=F32):
    return jax.ShapeDtypeStruct(shape, dtype)


def left_half(total, block, start, xv, ev, v3, q3):
    rank = v3.shape[0] // 3
    for i in range(total.shape[0] // rank * LANES // block):
        cut = pl.ds(pl.multiple_of(start + i * block, LANES), block)
        part = fold3(dot(v3[...], xv[:, cut], NN) + dot(q3[...], ev[cut, :], NT))
        for j in range(block // LANES):
            at = (i * (block // LANES) + j) * rank
            total[at : at + rank, :] = part[:, j * LANES : (j + 1) * LANES]


def put_chips(chips, ids, total, out):
    size = out.shape[0] // chips
    for chip in range(chips):
        start = pl.multiple_of((chip ^ ids[1]) * size, 8)
        out[chip * size : (chip + 1) * size, :] = total[pl.ds(start, size), :]


def cuts_of(block, start, half):
    return [pl.ds(pl.multiple_of(start + i * block, LANES), block) for i in range(half // block)]


def load_kernel(cores, block, ids, e_hbm, ev, sem):
    half = ev.shape[0] // cores
    cut = cuts_of(block, (1 - ids[0]) * half, half)[0]
    copy = pltpu.make_async_copy(e_hbm.at[0, cut, :], ev.at[cut, :], sem)
    copy.start()
    copy.wait()


def first_kernel(cores, chips, block, ids, x_hbm, e_hbm, y, q, e_in, send, xv, ev, v3, q3, total, sem):
    half = xv.shape[1] // cores
    theirs, own = cuts_of(block, (1 - ids[0]) * half, half), cuts_of(block, ids[0] * half, half)
    count = len(own)
    x_copies, e_copies = [], []
    for i, cut in enumerate(theirs + own):
        x_copies.append(pltpu.make_async_copy(x_hbm.at[:, cut], xv.at[:, cut], sem.at[2 * i]))
        if i > 0:
            e_copies.append(pltpu.make_async_copy(e_hbm.at[0, cut, :], ev.at[cut, :], sem.at[2 * i + 1]))
    for copy in e_copies[: count - 1] + x_copies + e_copies[count - 1 :]:
        copy.start()
    q3[...] = split3(q[...])
    rank = q.shape[0]
    tiles = block // LANES
    for i, cut in enumerate(theirs):
        if i > 0:
            e_copies[i - 1].wait()
        part = fold3(dot(q3[...], (e_in if i == 0 else ev)[cut, :], NT))
        for j in range(tiles):
            at = (i * tiles + j) * rank
            total[at : at + rank, :] = part[:, j * LANES : (j + 1) * LANES]
        if i == 0:
            v3[...] = split3(fold3(dot(q3[...], y[...], NT)))
    for i, cut in enumerate(theirs):
        x_copies[i].wait()
        part = fold3(dot(v3[...], xv[:, cut], NN))
        for j in range(tiles):
            at = (i * tiles + j) * rank
            total[at : at + rank, :] += part[:, j * LANES : (j + 1) * LANES]
    put_chips(chips, ids, total, send)
    for copy in x_copies[count:] + e_copies[count - 1 :]:
        copy.wait()


def second_kernel(chips, block, ids, xv, ev, v3, q3, keep, total):
    left_half(total, block, ids[0] * (total.shape[0] // (v3.shape[0] // 3) * LANES), xv, ev, v3, q3)
    put_chips(chips, ids, total, keep)


def sum_kernel(count, *refs):
    ins, outs = refs[:count], refs[count:]
    size = outs[0].shape[0]
    for k, out in enumerate(outs):
        rows = pl.ds(k * size, size)
        total = ins[0][rows, :]
        for other in ins[1:]:
            total = total + other[rows, :]
        out[...] = total


def add_up(ins, pieces):
    rows = ins[0].shape[0]
    shape = vmem((rows // pieces, LANES))
    return call(
        functools.partial(sum_kernel, len(ins)), [shape] * pieces, [VM] * len(ins), [VM] * pieces, [], ins, 10**7, 8
    )


def merge_kernel(span, xv, yv, ev, merged, parts):
    for i in range(ev.shape[0] // span):
        cut = slice(i * span, (i + 1) * span)
        block = dot(xv[:, cut], yv[...], TN) + ev[cut, :].astype(F32)
        merged[cut, :] = block
        high = block.astype(BF16)
        parts[2 * i * span : (2 * i + 1) * span, :] = high
        parts[(2 * i + 1) * span : (2 * i + 2) * span, :] = (block - high.astype(F32)).astype(BF16)


def chunk_of(chips, ids, where):
    return (where[0] ^ ids[0]) * chips + (where[1] ^ ids[1])


def split_chunks(parts, p3):
    rank = p3.shape[0] // 3
    for i in range(len(parts) * parts[0].shape[0] // rank):
        part, c = parts[i * rank // parts[0].shape[0]], i % (parts[0].shape[0] // rank)
        p3[:, i * LANES : (i + 1) * LANES] = split3(part[c * rank : (c + 1) * rank, :])


def add_chunks(chips, places, ids, p3, merged2, columns, t):
    span = p3.shape[1] // len(places)
    for i, where in enumerate(places):
        rows = pl.ds(pl.multiple_of(chunk_of(chips, ids, where) * (2 * span), 16), 2 * span)
        mine = p3[:, i * span : (i + 1) * span]
        new = dot(jnp.concatenate([mine, mine], axis=1), merged2[rows, columns], NN)
        t = new if t is None else t + new
    return t


def chunk_kernel(chips, places, first, ids, *refs):
    parts, rest = refs[: len(places)], refs[len(places) :]
    merged2, (p3, t) = rest[0], rest[-2:]
    split_chunks(parts, p3)
    t[...] = add_chunks(chips, places, ids, p3, merged2, slice(None), None if first else rest[1][...])


def half_of(chips, places, core, ids, p3, merged2, before, out):
    rank = p3.shape[0] // 3
    wide = out.shape[0] // rank * LANES
    columns = pl.ds(pl.multiple_of(core * wide, LANES), wide)
    right = fold3(add_chunks(chips, places, ids, p3, merged2, columns, before[:, columns]))
    for c in range(wide // LANES):
        out[c * rank : (c + 1) * rank, :] = right[:, c * LANES : (c + 1) * LANES]


def send_kernel(chips, places, ids, *refs):
    merged2, before, p3, send = refs[len(places) :]
    split_chunks(refs[: len(places)], p3)
    half_of(chips, places, 1 - ids[0], ids, p3, merged2, before, send)


def keep_kernel(chips, places, ids, p3, merged2, before, keep):
    half_of(chips, places, ids[0], ids, p3, merged2, before, keep)


def gram_kernel(*refs):
    gram = refs[-1]
    rank = gram.shape[0]
    full = sum(dot(p3[...], p3[...], NT) for p3 in refs[:-1])
    full = fold3(full)
    gram[...] = full[:, :rank] + full[:, rank : 2 * rank] + full[:, 2 * rank :]


def factor_kernel(gram, lower_inv):
    rank = gram.shape[0]
    n = 8
    row = lax.broadcasted_iota(jnp.int32, (rank, rank), 0)
    lane = lax.broadcasted_iota(jnp.int32, (rank, rank), 1)
    eye = jnp.where(lane == row, 1.0, 0.0).astype(F32)
    work = jnp.concatenate([eye, gram[...]], axis=1)
    groups = [work[n * g : n * g + n, :] for g in range(rank // n)]
    wide = (n, 2 * rank)
    def column(x, k):
        return jnp.broadcast_to(x[:, rank + k : rank + k + 1], wide)
    def line(x, i):
        return jnp.broadcast_to(x[i : i + 1, :], wide)
    sub = lax.broadcasted_iota(jnp.int32, wide, 0)
    for g in range(rank // n):
        base = n * g
        cols = [column(groups[g], base + j) for j in range(n)]
        b = {(i, j): line(cols[j], i) for j in range(n) for i in range(j, n)}
        low, inv = {}, []
        for s in range(n):
            inv.append(1.0 / b[s, s])
            for i in range(s + 1, n):
                low[i, s] = b[i, s] * inv[s]
            for j in range(s + 1, n):
                for i in range(j, n):
                    b[i, j] = b[i, j] - low[i, s] * b[j, s]
        rows = []
        for i in range(n):
            r = line(groups[g], i)
            for s in range(i):
                r = r - low[i, s] * rows[s]
            rows.append(r)
        for h in range(g + 1, rank // n):
            x = [column(groups[h], base + s) for s in range(n)]
            for s in range(n):
                for t in range(s):
                    x[s] = x[s] - low[s, t] * x[t]
            new = groups[h]
            for s in range(n):
                new = new - (x[s] * inv[s]) * rows[s]
            groups[h] = new
        out = jnp.zeros(wide, F32)
        for i in range(n):
            out = jnp.where(sub == i, rows[i] * jnp.sqrt(inv[i]), out)
        lower_inv[base : base + n, :] = out[:, :rank]


def hat_kernel(cores, chips, places, ids, *refs):
    p3s, (lower_inv, out, hat3, p_hat, sem) = refs[:-5], refs[-5:]
    rank = lower_inv.shape[0]
    inv3 = split3(lower_inv[...])
    at = 0
    for p3 in p3s:
        full = dot(inv3, p3[:rank, :], NN)
        mids = dot(inv3[: 2 * rank], p3[rank : 2 * rank, :], NN)
        hats = fold3(full) + (mids[:rank] + mids[rank:]) + dot(inv3[:rank], p3[2 * rank :, :], NN)
        span = p_hat.shape[1] // (cores * chips)
        for i in range(p3.shape[1] // span):
            start = chunk_of(chips, ids, places[at]) * span
            at += 1
            hat = hats[:, i * span : (i + 1) * span]
            p_hat[:, pl.ds(pl.multiple_of(start, LANES), span)] = hat
            for c in range(span // LANES):
                turned = hat[:, c * LANES : (c + 1) * LANES].T
                high = turned.astype(BF16)
                low = (turned - high.astype(F32)).astype(BF16)
                rows = pl.ds(pl.multiple_of(start + c * LANES, LANES), LANES)
                hat3[rows, :] = jnp.concatenate([high, low, high], axis=1)
    copy = pltpu.make_async_copy(p_hat, out, sem)
    copy.start()
    copy.wait()


def last_kernel(devices, block, ids, keep, other, lower_inv, hat3, merged, new_errors, q_mean, total, out, q_out, sem):
    rank = lower_inv.shape[0]
    half = keep.shape[0]
    total[pl.ds(pl.multiple_of(ids[0] * half, 8), half), :] = keep[...]
    if other is not None:
        total[pl.ds(pl.multiple_of((1 - ids[0]) * half, 8), half), :] = other[...]
    wide = jnp.concatenate([total[c * rank : (c + 1) * rank, :] for c in range(total.shape[0] // rank)], axis=1)
    a, b = split3(lower_inv[...]), split3(wide)
    ah, am, al = a[:rank], a[rank : 2 * rank], a[2 * rank :]
    bh, bm, bl = b[:rank], b[rank : 2 * rank], b[2 * rank :]
    right = dot(jnp.concatenate([ah, ah, am, ah, al, am], axis=1), jnp.concatenate([bh, bm, bh, bl, bh, bm], axis=0), NN)
    right = right / devices
    high = right.astype(BF16)
    low = (right - high.astype(F32)).astype(BF16)
    q3 = jnp.concatenate([high, high, low], axis=0)
    q_out[...] = right
    copies = [pltpu.make_async_copy(q_out, q_mean, sem.at[0])]
    copies[0].start()
    for i in range(merged.shape[0] // block):
        cut = pl.ds(i * block, block)
        out[cut, :] = (merged[cut, :] - dot(hat3[cut, :], q3, NN)).astype(BF16)
        copies.append(pltpu.make_async_copy(out.at[cut, :], new_errors.at[0, cut, :], sem.at[1 + i]))
        copies[1 + i].start()
    for copy in copies:
        copy.wait()


def exchange(parts, axis, size):
    return [parts[0]] + [swap(parts[k], axis, size, k) for k in range(1, size)]


def swap(x, axis, size, by):
    return lax.ppermute(x, axis, [(i, i ^ by) for i in range(size)])


def body(sizes, *args):
    return step(sizes, *args)


def step(sizes, inputs, cotangent, errors, previous_q):
    cores, chips, groups, cuts = sizes
    tokens, depth = inputs.shape
    width, rank = previous_q.shape
    devices = cores * chips * groups * cuts
    rows = depth * rank // LANES
    span = depth // (cores * chips)
    block = next(b for b in (512, 384, 256, LANES) if depth // cores % b == 0)
    tail = block // 2
    ids = jnp.stack([lax.axis_index("core"), lax.axis_index("chip")]).astype(jnp.int32)
    half = vmem((rows // cores, LANES))
    total = pltpu.VMEM((rows // cores, LANES), F32)
    held = vmem((depth, width), BF16)
    blocks = depth // cores // block
    ev = call(
        functools.partial(load_kernel, cores, block),
        held,
        [SM, HBM],
        VM,
        [pltpu.SemaphoreType.DMA],
        (ids, errors),
        10**9,
        49,
    )
    send, xv, ev, v3, q3 = call(
        functools.partial(first_kernel, cores, chips, block),
        [half, vmem((tokens, depth), BF16), held, vmem((3 * rank, tokens), BF16), vmem((3 * rank, width), BF16)],
        [SM, HBM, HBM] + [VM] * 3,
        [VM] * 5,
        [total, pltpu.SemaphoreType.DMA((4 * blocks,))],
        (ids, inputs, errors, cotangent, previous_q.T, ev),
        10**9,
        46,
        {5: 2},
    )
    got = swap(send, "core", cores, 1)
    keep = call(
        functools.partial(second_kernel, chips, block),
        half,
        [SM] + [VM] * 4,
        VM,
        [total],
        (ids, xv, ev, v3, q3),
        10**9,
        8,
    )
    parts = add_up([keep, got], chips)
    parts = add_up(exchange(parts, "chip", chips), 1)
    if groups > 1:
        parts = add_up(exchange(parts * groups, "group", groups), 1)
    parts = add_up(exchange(parts * cuts, "cuts", cuts), 1)
    parts = exchange(parts * chips, "chip", chips)
    parts = parts + [swap(part, "core", cores, 1) for part in parts]

    merged, merged2 = call(
        functools.partial(merge_kernel, span),
        [vmem((depth, width)), vmem((2 * depth, width), BF16)],
        [VM] * 3,
        [VM] * 2,
        [],
        (xv, cotangent, ev),
        10**9,
        8,
    )
    places = [(core, chip) for core in range(cores) for chip in range(chips)]
    batches = [[0], [chips, *range(1, chips)], list(range(chips + 1, 2 * chips))]
    share = vmem((width * rank // LANES // cores, LANES))
    t, p3s, order = [], [], []
    for at, batch in enumerate(batches):
        where = [places[k] for k in batch]
        arrived = [parts[k] for k in batch]
        end = at == len(batches) - 1
        p3, more = call(
            functools.partial(send_kernel, chips, where) if end else functools.partial(chunk_kernel, chips, where, at == 0),
            [vmem((3 * rank, span * len(batch)), BF16), share if end else vmem((3 * rank, width))],
            [SM] + [VM] * (len(batch) + 1 + len(t)),
            [VM] * 2,
            [],
            (ids, *arrived, merged2, *t),
            10**8,
            8,
        )
        p3s.append(p3)
        order += where
        if not end:
            t = [more]
    send = more
    keep = call(
        functools.partial(keep_kernel, chips, where),
        share,
        [SM] + [VM] * 3,
        VM,
        [],
        (ids, p3s[-1], merged2, *t),
        10**8,
        8,
    )
    got = swap(send, "core", cores, 1)
    part = add_up([keep, got], 1)[0]
    part = add_up(exchange([part] * chips, "chip", chips), 1)[0]
    if groups > 1:
        part = add_up(exchange([part] * groups, "group", groups), 1)[0]
    part = add_up(exchange([part] * cuts, "cuts", cuts), 1)[0]
    other = swap(part, "core", cores, 1)

    gram = call(gram_kernel, vmem((rank, rank)), [VM] * len(p3s), VM, [], p3s, 10**8, 8)
    lower_inv = call(factor_kernel, vmem((rank, rank)), [VM], VM, [], (gram,), 10**9, 8)
    p_hat, hat3 = call(
        functools.partial(hat_kernel, cores, chips, order),
        [vmem((rank, depth)), vmem((depth, 3 * rank), BF16)],
        [SM] + [VM] * (len(p3s) + 1),
        [HBM, VM],
        [pltpu.VMEM((rank, depth), F32), pltpu.SemaphoreType.DMA],
        (ids, *p3s, lower_inv),
        10**9,
        8,
    )
    new_errors, q_mean = call(
        functools.partial(last_kernel, devices, tail),
        [vmem((1, depth, width), BF16), vmem((rank, width))],
        [SM] + [VM] * 5,
        [HBM] * 2,
        [
            pltpu.VMEM((width * rank // LANES, LANES), F32),
            pltpu.VMEM((depth, width), BF16),
            pltpu.VMEM((rank, width), F32),
            pltpu.SemaphoreType.DMA((1 + depth // tail,)),
        ],
        (ids, part, other, lower_inv, hat3, merged),
        10**9,
        16,
    )
    return (new_errors, p_hat.T, q_mean.T)


def solution(mesh):
    cuts, dev = mesh.shape["cuts"], mesh.shape["dev"]
    cores = 2
    every = ("cuts", "group", "chip", "core")

    def program(inputs, cotangent, errors, previous_q):
        columns = inputs.shape[1] // (cores * LANES)
        chips = next(n for n in range(dev // cores, 0, -1) if dev // cores % n == 0 and columns % n == 0)
        groups = dev // (cores * chips)
        fine = Mesh(mesh.devices.reshape(cuts, groups, chips, cores), every)
        run = jax.shard_map(
            functools.partial(body, (cores, chips, groups, cuts)),
            mesh=fine,
            in_specs=(P(every, None), P(every, None), P(every, None, None), P()),
            out_specs=(P(every, None, None), P(), P()),
            check_vma=False,
        )
        return run(inputs, cotangent, errors, previous_q)

    return program
```
